32 devices in a mesh: dp: 4 (over x, core), seq: 4 (over z), tensor: 2 (over y).
Axes of the slice: x: 2, y: 2, z: 4, core: 2. Of those that a mesh axis runs over, the one named last changes fastest.
Arguments:
- vit_out: bfloat16 [4096, 3200], P(('dp', 'seq')), may hold values from -6 to 6
- ln_gain: float32 [3200], replicated, may hold values from 0.1 to 1.9
- ln_bias: float32 [3200], replicated, may hold values from -3 to 3
- proj_weight: bfloat16 [3200, 4, 2048], P(None, None, 'tensor'), may hold values from -0.109375 to 0.109375
- proj_bias: float32 [4, 2048], P(None, 'tensor'), may hold values from -3 to 3
- text_embed: bfloat16 [16384, 8192], P('dp', ('seq', 'tensor')), may hold values from -6 to 6
- norm_gain: float32 [8192], P(('seq', 'tensor')), may hold values from 0.1 to 1.9
- tile_dest: int32 [32, 1], replicated, may hold values from 0 to 3; in each aligned block of 8 rows (0 to 7, 8 to 15, ...) at most 4 rows name the same one
- tile_place: int32 [4, 32], replicated, may hold values from 0 to 31, each once within a row
Outputs:
- normed: bfloat16 [16384, 8192], P('dp', ('seq', 'tensor'))
The draws below stay inside these ranges and needn't reach their ends.
Inputs may be any that keep to these rules, and one draw needn't show every extreme that they name: `tile_dest`: in each aligned block of 8 rows (one encoder group's tiles) no replica is named more than 4 times, a bound that some block reaches. `tile_place`: each row is a permutation of 0 to 31.
All inputs are finite; a program needn't handle non-finite values.
Results may differ from the reference program's by a relative error of at most 0.0048.
Values may be sent and summed in bfloat16 or wider, within the bound.
A program may use at most 128 MiB of HBM per device.

```python
import math
import jax
import jax.numpy as jnp
import numpy as np
from jax import lax

VD = 3200
D = 8192
TILE = 128
SEQS = 4
SEQ_LEN = 1024
GROUP_TILES = 8
CAP = 4
POSITIONS = 32
N_DP = 4
N_SEQ = 4


def block_levels(key, extent, split, smallest, top_value):
    def one(dim, shards_of):
        steps = jax.random.uniform(jax.random.fold_in(jax.random.fold_in(key, 6), dim), (shards_of,), jnp.float32, smallest / len(split), top_value / len(split))
        return jnp.repeat(jnp.exp(steps), extent[dim] // shards_of).reshape((-1,) + (1,) * (len(extent) - dim - 1))

    loudness = one(*split[0])
    for cut in split[1:]:
        loudness = loudness * one(*cut)
    return loudness


def assign_block(rng, own, number, rows, count, top, most, slope):
    order = jax.random.permutation(rng, count)
    packed, common = shares(count, rows * top, most, slope, True), shares(count, rows * top, most, slope, False)
    places = jnp.arange(count)

    def named(lengths, turn):
        used = int((lengths > 0).sum())
        fixed = max(1, used // 4)
        passed = fixed + (places - fixed + turn * (used - fixed)) % max(1, count - fixed)
        return jnp.zeros((count,), jnp.int32).at[order[jnp.where(places < fixed, places, passed)]].set(jnp.asarray(lengths, jnp.int32))

    lengths = jnp.where(number % 4 == 0, named(packed, number // 4), named(common, number - number // 4 - 1))
    mixed = jax.random.permutation(jax.random.fold_in(own, 3), count)
    source_of, taker = mixed[0:count // 2 * 2:2], mixed[1:count // 2 * 2:2]
    room = jnp.minimum(lengths[source_of] - 1, most - lengths[taker]) // 2
    room = jnp.where((source_of == order[0]) | (taker == order[0]) | (lengths[taker] == 0), 0, jnp.maximum(room, 0))
    passed = jax.random.randint(jax.random.fold_in(own, 4), (count // 2,), 0, 1 << 20) % (room + 1)
    lengths = lengths.at[source_of].add(-passed).at[taker].add(passed)
    items = jnp.searchsorted(jnp.cumsum(lengths), jnp.arange(rows * top), side="right").astype(jnp.int32)
    grid = items.reshape(top, rows).T
    grid = grid[jax.random.permutation(jax.random.fold_in(own, 1), rows)]
    turn = jax.random.randint(jax.random.fold_in(own, 2), (rows, 1), 0, top)
    return jnp.take_along_axis(grid, (jnp.arange(top)[None, :] + turn) % top, axis=1)


def shares(amount, total, most, lean, full):
    portions = [(1 << 20) // math.isqrt(rank ** lean) + 1 for rank in range(1, amount + 1)]
    largest = most if full else min(most, max(-(-total // amount), total * portions[0] // sum(portions)))
    least = 1 if total - largest >= amount - 1 else 0
    counts, spare = [largest] + [least] * (amount - 1), total - largest - least * (amount - 1)
    while spare > 0:
        candidates = [i for i in range(1, amount) if counts[i] < largest] or [i for i in range(1, amount) if counts[i] < most]
        pool, remaining = sum([portions[i] for i in candidates]), spare
        for i in candidates:
            extra = min(most - counts[i], max(1, remaining * portions[i] // pool), spare)
            counts[i] = counts[i] + extra
            spare = spare - extra
    return np.array(counts)


def bell_draw(key, extent, deviation, reach, shards=(), kind=jnp.bfloat16):
    gain = block_levels(key, extent, shards, -0.22, 0.18) if shards else 1.0
    array = jax.random.normal(key, extent, jnp.float32) * deviation * gain
    return jnp.minimum(jnp.maximum(array, -reach), reach).astype(kind)


def setup_inputs(seed: int = 0) -> dict:
    arg_keys = jax.random.split(jax.random.key(seed), 10)
    vit_out = bell_draw(arg_keys[0], (N_DP * GROUP_TILES * TILE, VD), 1.0, 6.0, ((0, 16),))
    ln_gain = jnp.clip(1.0 + 0.18 * jax.random.normal(arg_keys[1], (VD,), jnp.float32), 0.1, 1.9)
    ln_bias = bell_draw(arg_keys[2], (VD,), 0.5, 3.0, (), jnp.float32)
    proj_weight = bell_draw(arg_keys[3], (VD, N_SEQ, D // N_SEQ), VD ** -0.5, 0.109375, ((2, 2),))
    proj_bias = bell_draw(arg_keys[4], (N_SEQ, D // N_SEQ), 0.5, 3.0, ((1, 2),), jnp.float32)
    text_embed = bell_draw(arg_keys[5], (N_DP * SEQS * SEQ_LEN, D), 1.0, 6.0, ((0, 4), (1, 8)))
    norm_gain = jnp.clip(1.0 + 0.18 * jax.random.normal(arg_keys[6], (D,), jnp.float32), 0.1, 1.9)
    tile_dest_keys = jax.random.split(jax.random.fold_in(arg_keys[7], 1), (N_DP * GROUP_TILES) // GROUP_TILES)
    tile_dest_turns = jax.random.permutation(jax.random.fold_in(arg_keys[7], 3), (N_DP * GROUP_TILES) // GROUP_TILES)
    tile_dest = jax.vmap(lambda own, number: assign_block(jax.random.fold_in(arg_keys[7], 2), own, number, GROUP_TILES, N_DP, 1, CAP, 2))(tile_dest_keys, tile_dest_turns).reshape((N_DP * GROUP_TILES, 1))
    tile_place = jax.vmap(lambda own: jax.random.permutation(own, POSITIONS))(jax.random.split(arg_keys[8], N_DP)).reshape((N_DP, POSITIONS)).astype(jnp.int32)
    return {"vit_out": vit_out, "ln_gain": ln_gain, "ln_bias": ln_bias, "proj_weight": proj_weight, "proj_bias": proj_bias, "text_embed": text_embed, "norm_gain": norm_gain, "tile_dest": tile_dest, "tile_place": tile_place}


def layer_norm(rows, ln_gain, ln_bias):
    values = rows.astype(jnp.float32)
    center = values - lax.optimization_barrier(jnp.mean(values, axis=-1, keepdims=True))
    spread = lax.optimization_barrier(jnp.mean(center * center, axis=-1, keepdims=True))
    return (center * lax.rsqrt(spread + 1e-06) * ln_gain + ln_bias).astype(jnp.bfloat16)

def arrival_ranks(destination, replicas):
    onehot = (destination[:, None] == jnp.arange(replicas, dtype=jnp.int32)[None, :]).astype(jnp.int32)
    before = jnp.cumsum(onehot, axis=0) - onehot
    return lax.optimization_barrier(jnp.sum(before * onehot, axis=1))

def reference(vit_out, ln_gain, ln_bias, proj_weight, proj_bias, text_embed, norm_gain, tile_dest, tile_place):
    weights = proj_weight.reshape(VD, D)
    bias_flat = proj_bias.reshape(D)

    def project(rows):
        normed_in = layer_norm(rows, ln_gain, ln_bias)
        hidden = jnp.dot(normed_in, weights, preferred_element_type=jnp.float32) + bias_flat
        return hidden.astype(jnp.bfloat16)
    projected = lax.map(project, vit_out.reshape(N_DP, GROUP_TILES * TILE, VD))
    tiles = projected.reshape(N_DP * GROUP_TILES, TILE, D)
    total_tiles = N_DP * GROUP_TILES
    destination = tile_dest[:, 0].astype(jnp.int32)
    ranks = arrival_ranks(destination, N_DP)
    slots = tile_place[destination, ranks].astype(jnp.int32)
    target = destination * POSITIONS + slots
    source_tile = jnp.full((N_DP * POSITIONS,), -1, jnp.int32).at[target].set(jnp.arange(total_tiles, dtype=jnp.int32))
    source_tile = source_tile.reshape(N_DP, POSITIONS)
    text_tiles = text_embed.reshape(N_DP, POSITIONS, TILE, D)

    def assemble(items):
        sources, text_part = items
        picked = tiles[jnp.clip(sources, 0, total_tiles - 1)]
        assembled = jnp.where((sources >= 0)[:, None, None], picked, text_part).reshape(POSITIONS * TILE, D)
        values = assembled.astype(jnp.float32)
        mean_square = lax.optimization_barrier(jnp.sum(values * values, axis=-1)) / D
        return (values * lax.rsqrt(mean_square + 1e-05)[:, None] * norm_gain).astype(jnp.bfloat16)
    result = lax.map(assemble, (source_tile, text_tiles))
    return result.reshape(N_DP * POSITIONS * TILE, D)
```

```python
import functools

import jax
import jax.numpy as jnp
from jax import lax
from jax.experimental import pallas as pl
from jax.experimental.pallas import tpu as pltpu
from jax.sharding import PartitionSpec as P

TILE = 128
CORES = 2
STAT_ROWS = 8
MESH = pl.DeviceIdType.MESH


def layer_norm(rows, ln_gain, ln_bias):
    values = rows.astype(jnp.float32)
    center = values - jnp.mean(values, axis=-1, keepdims=True)
    spread = jnp.mean(center * center, axis=-1, keepdims=True)
    return (center * lax.rsqrt(spread + 1e-06) * ln_gain + ln_bias).astype(jnp.bfloat16)


def send_order(place, owners):
    toward = 1 if place < owners // 2 else -1
    steps = [0, 1] + list(range(2, owners))
    return [(place + toward * step) % owners for step in steps]


def arrival_order(place, owners):
    return sorted(range(owners), key=lambda other: (abs(other - place), -abs(2 * other - owners + 1)))


def lookup(index, table):
    value = jnp.int32(table[0])
    for entry in range(1, len(table)):
        value = jnp.where(index == entry, jnp.int32(table[entry]), value)
    return value


def exchange_kernel(
    sizes,
    proj_ref,
    stat_ref,
    out_ref,
    text_ref,
    vision_ref,
    y_land,
    z_land,
    d_land,
    local_sem,
    zs_sem,
    zr_sem,
    xs_sem,
    xr_sem,
    cs_sem,
    cr_sem,
    ys_sem,
    yr_sem,
    zss_sem,
    zsr_sem,
    ds_sem,
    dr_sem,
):
    replicas, owners, splits, tiles = sizes
    chips = replicas // CORES
    mine = lax.axis_index("dp")
    place = lax.axis_index("seq")
    half = lax.axis_index("tensor")
    chip = mine // CORES
    core = mine % CORES
    partner = chip * CORES + 1 - core

    barrier = pltpu.get_barrier_semaphore()
    for step in range(1, replicas):
        pl.semaphore_signal(
            barrier, inc=1, device_id={"dp": (mine + step) % replicas}, device_id_type=MESH
        )
    for step in range(1, owners):
        pl.semaphore_signal(
            barrier, inc=1, device_id={"seq": (place + step) % owners}, device_id_type=MESH
        )
    for step in range(1, splits):
        pl.semaphore_signal(
            barrier, inc=1, device_id={"tensor": (half + step) % splits}, device_id_type=MESH
        )
    pl.semaphore_wait(barrier, replicas + owners + splits - 3)

    sends = []

    def push(src, dst, send_sem, recv_sem, device):
        copy = pltpu.make_async_remote_copy(
            src_ref=src,
            dst_ref=dst,
            send_sem=send_sem,
            recv_sem=recv_sem,
            device_id=device,
            device_id_type=MESH,
        )
        copy.start()
        sends.append(copy)

    def arrived(dst, send_sem, recv_sem, device):
        pltpu.make_async_remote_copy(
            src_ref=dst,
            dst_ref=dst,
            send_sem=send_sem,
            recv_sem=recv_sem,
            device_id=device,
            device_id_type=MESH,
        ).wait_recv()

    y_sends = []
    for step in range(1, splits):
        other = (half + step) % splits
        push(
            stat_ref,
            y_land.at[half],
            ys_sem.at[step],
            yr_sem.at[half],
            {"tensor": other},
        )

    targets = [
        lookup(place, [send_order(p, owners)[k] for p in range(owners)]) for k in range(owners)
    ]
    sources = [
        lookup(place, [arrival_order(p, owners)[k] for p in range(owners)]) for k in range(owners)
    ]

    for k in range(1, owners):
        for tile in range(tiles):
            push(
                proj_ref.at[targets[k], tile],
                out_ref.at[mine, place, tile],
                zs_sem.at[k, tile],
                zr_sem.at[place, tile],
                {"seq": targets[k]},
            )

    def spread(src, k, tile):
        owner = sources[k]
        for step in range(1, chips):
            other = (chip + step) % chips
            push(
                src,
                out_ref.at[mine, owner, tile],
                xs_sem.at[step, k, tile],
                xr_sem.at[chip, owner, tile],
                {"dp": other * CORES + core},
            )
        push(
            src,
            out_ref.at[mine, owner, tile],
            cs_sem.at[0, k, tile],
            cr_sem.at[chip, owner, tile],
            {"dp": partner},
        )

    def relay(k, tile):
        owner = sources[k]
        for step in range(1, chips):
            other = (chip + chips - step) % chips
            origin = other * CORES + core
            block = out_ref.at[origin, owner, tile]
            arrived(block, xs_sem.at[step, k, tile], xr_sem.at[other, owner, tile], {"dp": origin})
            push(
                block,
                block,
                cs_sem.at[step, k, tile],
                cr_sem.at[other, owner, tile],
                {"dp": partner},
            )

    for tile in range(tiles):
        spread(proj_ref.at[place, tile], 0, tile)
    keep = pltpu.make_async_copy(proj_ref.at[place], out_ref.at[mine, place], local_sem)
    keep.start()

    total = stat_ref[...]
    for step in range(1, splits):
        other = (half + step) % splits
        arrived(y_land.at[other], ys_sem.at[step], yr_sem.at[other], {"tensor": other})
        total = total + y_land[other]
    z_land[place] = total
    for step in range(1, owners):
        other = (place + step) % owners
        push(
            z_land.at[place],
            z_land.at[place],
            zss_sem.at[step],
            zsr_sem.at[place],
            {"seq": other},
        )

    def statistics():
        text_total = jnp.zeros(text_ref.shape, jnp.float32)
        for step in range(1, owners):
            other = (place + step) % owners
            arrived(z_land.at[other], zss_sem.at[step], zsr_sem.at[other], {"seq": other})
        for owner in range(owners):
            text_total = text_total + z_land[owner, STAT_ROWS:, :]
            d_land[mine, owner] = z_land[owner, :STAT_ROWS, :]
        text_ref[...] = text_total
        for step in range(1, replicas):
            other = (mine + step) % replicas
            push(
                d_land.at[mine],
                d_land.at[mine],
                ds_sem.at[step],
                dr_sem.at[mine],
                {"dp": other},
            )

    for k in range(1, owners):
        for tile in range(tiles):
            arrived(
                out_ref.at[mine, sources[k], tile],
                zs_sem.at[k, tile],
                zr_sem.at[sources[k], tile],
                {"seq": sources[k]},
            )
            spread(out_ref.at[mine, sources[k], tile], k, tile)
        if k == owners - 1:
            statistics()
        for tile in range(tiles):
            relay(k - 1, tile)
    for tile in range(tiles):
        relay(owners - 1, tile)

    for step in range(1, replicas):
        other = (mine + step) % replicas
        arrived(d_land.at[other], ds_sem.at[step], dr_sem.at[other], {"dp": other})
    vision_ref[...] = d_land[...]
    for k in range(owners):
        for other in range(chips):
            origin = other * CORES + 1 - core
            for tile in range(tiles):
                arrived(
                    out_ref.at[origin, sources[k], tile],
                    cs_sem.at[0, k, tile],
                    cr_sem.at[other, sources[k], tile],
                    {"dp": partner},
                )
    keep.wait()
    for copy in sends:
        copy.wait_send()


def exchange(blocks, stats, sizes):
    replicas, owners, splits, tiles = sizes
    chips = replicas // CORES
    columns = blocks.shape[-1]
    rows = stats.shape[0]
    dma = pltpu.SemaphoreType.DMA
    return pl.pallas_call(
        functools.partial(exchange_kernel, sizes),
        out_shape=(
            jax.ShapeDtypeStruct((replicas, owners, tiles, TILE, columns), jnp.bfloat16),
            jax.ShapeDtypeStruct((rows - STAT_ROWS, TILE), jnp.float32),
            jax.ShapeDtypeStruct((replicas, owners, STAT_ROWS, TILE), jnp.float32),
        ),
        in_specs=[pl.BlockSpec(memory_space=pltpu.VMEM)] * 2,
        out_specs=(
            pl.BlockSpec(memory_space=pl.ANY),
            pl.BlockSpec(memory_space=pltpu.VMEM),
            pl.BlockSpec(memory_space=pltpu.VMEM),
        ),
        scratch_shapes=[
            pltpu.VMEM((splits, rows, TILE), jnp.float32),
            pltpu.VMEM((owners, rows, TILE), jnp.float32),
            pltpu.VMEM((replicas, owners, STAT_ROWS, TILE), jnp.float32),
            dma,
            dma((owners, tiles)),
            dma((owners, tiles)),
            dma((chips, owners, tiles)),
            dma((chips, owners, tiles)),
            dma((chips, owners, tiles)),
            dma((chips, owners, tiles)),
            dma((splits,)),
            dma((splits,)),
            dma((owners,)),
            dma((owners,)),
            dma((replicas,)),
            dma((replicas,)),
        ],
        compiler_params=pltpu.CompilerParams(collective_id=0, has_side_effects=True),
        name="exchange",
    )(blocks, stats)


def place_kernel(group, width, source_ref, *refs):
    picked = refs[:group]
    text_ref, text_sum, vision_sum, gain_ref, out_ref = refs[group:]
    first = pl.program_id(0) * group
    gain = gain_ref[...]
    for item in range(group):
        source = source_ref[first + item]
        rows = slice(item * TILE, (item + 1) * TILE)

        def scaled(values, squares):
            scale = lax.rsqrt(squares / width + 1e-05)
            column = jnp.broadcast_to(scale, (TILE, TILE)).T
            for start in range(0, out_ref.shape[1], TILE):
                lanes = slice(start, start + TILE)
                out_ref[rows, lanes] = (
                    values[:, lanes].astype(jnp.float32) * column * gain[:, lanes]
                ).astype(jnp.bfloat16)

        @pl.when(source >= 0)
        def _():
            scaled(picked[item][0], vision_sum[pl.ds(source, 1), :])

        @pl.when(source < 0)
        def _():
            scaled(text_ref[rows, :], text_sum[pl.ds(first + item, 1), :])


def place(source_tile, gathered, text_embed, text_sum, vision_sum, norm_gain, width):
    positions = source_tile.shape[0]
    group = 4
    columns = text_embed.shape[1]

    def pick(item):
        return lambda step, source: (jnp.maximum(source[step * group + item], 0), 0, 0)

    whole = lambda step, source: (0, 0)
    return pl.pallas_call(
        functools.partial(place_kernel, group, width),
        grid_spec=pltpu.PrefetchScalarGridSpec(
            num_scalar_prefetch=1,
            grid=(positions // group,),
            in_specs=[pl.BlockSpec((1, TILE, columns), pick(item)) for item in range(group)]
            + [
                pl.BlockSpec((group * TILE, columns), lambda step, source: (step, 0)),
                pl.BlockSpec(text_sum.shape, whole),
                pl.BlockSpec(vision_sum.shape, whole),
                pl.BlockSpec((1, columns), whole),
            ],
            out_specs=pl.BlockSpec((group * TILE, columns), lambda step, source: (step, 0)),
        ),
        out_shape=jax.ShapeDtypeStruct(text_embed.shape, jnp.bfloat16),
        name="place",
    )(source_tile, *([gathered] * group), text_embed, text_sum, vision_sum, norm_gain[None, :])


def local(
    vit_out, ln_gain, ln_bias, proj_weight, proj_bias, text_embed, norm_gain, tile_dest, tile_place
):
    replicas = lax.axis_size("dp")
    owners = lax.axis_size("seq")
    splits = lax.axis_size("tensor")
    mine = lax.axis_index("dp")
    local_rows = vit_out.shape[0]
    width_in = vit_out.shape[1]
    columns = proj_weight.shape[2]
    positions = tile_place.shape[1]
    total_tiles = tile_dest.shape[0]
    tiles = local_rows // TILE
    sizes = (replicas, owners, splits, tiles)

    normed_in = layer_norm(vit_out, ln_gain, ln_bias)
    hidden = jnp.dot(
        normed_in,
        proj_weight.reshape(width_in, owners * columns),
        preferred_element_type=jnp.float32,
    ) + proj_bias.reshape(-1)
    projected = hidden.astype(jnp.bfloat16)
    own_squares = jnp.sum(jnp.square(projected.astype(jnp.float32)), axis=-1)
    text_squares = jnp.sum(jnp.square(text_embed.astype(jnp.float32)), axis=-1)
    stats = jnp.concatenate(
        [
            jnp.pad(own_squares.reshape(tiles, TILE), ((0, STAT_ROWS - tiles), (0, 0))),
            text_squares.reshape(positions, TILE),
        ]
    )
    blocks = projected.reshape(tiles, TILE, owners, columns).transpose(2, 0, 1, 3)
    gathered, text_sum, vision_sum = exchange(blocks, stats, sizes)

    named = tile_dest[:, 0] == mine
    earlier = jnp.arange(total_tiles)[None, :] < jnp.arange(total_tiles)[:, None]
    ranks = jnp.sum((earlier & named[None, :]).astype(jnp.int32), axis=1)
    place_row = lax.dynamic_index_in_dim(tile_place, mine, 0, keepdims=False)
    numbers = jnp.arange(positions, dtype=jnp.int32)
    order = jnp.sum(
        jnp.where(place_row[None, :] == numbers[:, None], numbers[None, :], 0), axis=1
    )
    matches = named[None, :] & (ranks[None, :] == order[:, None])
    source_tile = jnp.max(
        jnp.where(matches, jnp.arange(total_tiles, dtype=jnp.int32)[None, :], -1), axis=1
    )
    return place(
        source_tile,
        gathered.reshape(total_tiles, TILE, columns),
        text_embed,
        text_sum,
        vision_sum[:, :, :tiles, :].reshape(total_tiles, TILE),
        norm_gain,
        norm_gain.shape[0] * owners * splits,
    )


def solution(mesh):
    placed = (
        P(("dp", "seq"), None),
        P(),
        P(),
        P(None, None, "tensor"),
        P(None, "tensor"),
        P("dp", ("seq", "tensor")),
        P(("seq", "tensor")),
        P(),
        P(),
    )
    return jax.shard_map(
        local, mesh=mesh, in_specs=placed, out_specs=P("dp", ("seq", "tensor")), check_vma=False
    )
```

```python
import functools

import jax
import jax.numpy as jnp
from jax import lax
from jax.experimental import pallas as pl
from jax.experimental.pallas import tpu as pltpu
from jax.sharding import PartitionSpec as P

TILE = 128
CORES = 2
STAT_ROWS = 8
DEPTH = 640
MESH = pl.DeviceIdType.MESH


def layer_norm(rows, ln_gain, ln_bias):
    values = rows.astype(jnp.float32)
    center = values - jnp.mean(values, axis=-1, keepdims=True)
    spread = jnp.mean(center * center, axis=-1, keepdims=True)
    return (center * lax.rsqrt(spread + 1e-06) * ln_gain + ln_bias).astype(jnp.bfloat16)


def send_order(place, owners):
    toward = 1 if place < owners // 2 else -1
    steps = [0, 1] + list(range(2, owners))
    return [(place + toward * step) % owners for step in steps]


def arrival_order(place, owners):
    return sorted(range(owners), key=lambda other: (abs(other - place), -abs(2 * other - owners + 1)))


def lookup(index, table):
    value = jnp.int32(table[0])
    for entry in range(1, len(table)):
        value = jnp.where(index == entry, jnp.int32(table[entry]), value)
    return value


def exchange_kernel(
    sizes,
    proj_ref,
    stat_ref,
    out_ref,
    text_ref,
    vision_ref,
    y_land,
    z_land,
    d_land,
    local_sem,
    zs_sem,
    zr_sem,
    xs_sem,
    xr_sem,
    cs_sem,
    cr_sem,
    ys_sem,
    yr_sem,
    zss_sem,
    zsr_sem,
    ds_sem,
    dr_sem,
):
    replicas, owners, splits, tiles = sizes
    chips = replicas // CORES
    mine = lax.axis_index("dp")
    place = lax.axis_index("seq")
    half = lax.axis_index("tensor")
    chip = mine // CORES
    core = mine % CORES
    partner = chip * CORES + 1 - core

    barrier = pltpu.get_barrier_semaphore()
    for step in range(1, replicas):
        pl.semaphore_signal(
            barrier, inc=1, device_id={"dp": (mine + step) % replicas}, device_id_type=MESH
        )
    for step in range(1, owners):
        pl.semaphore_signal(
            barrier, inc=1, device_id={"seq": (place + step) % owners}, device_id_type=MESH
        )
    for step in range(1, splits):
        pl.semaphore_signal(
            barrier, inc=1, device_id={"tensor": (half + step) % splits}, device_id_type=MESH
        )
    pl.semaphore_wait(barrier, replicas + owners + splits - 3)

    sends = []

    def push(src, dst, send_sem, recv_sem, device):
        copy = pltpu.make_async_remote_copy(
            src_ref=src,
            dst_ref=dst,
            send_sem=send_sem,
            recv_sem=recv_sem,
            device_id=device,
            device_id_type=MESH,
        )
        copy.start()
        sends.append(copy)

    def arrived(dst, send_sem, recv_sem, device):
        pltpu.make_async_remote_copy(
            src_ref=dst,
            dst_ref=dst,
            send_sem=send_sem,
            recv_sem=recv_sem,
            device_id=device,
            device_id_type=MESH,
        ).wait_recv()

    y_sends = []
    for step in range(1, splits):
        other = (half + step) % splits
        push(
            stat_ref,
            y_land.at[half],
            ys_sem.at[step],
            yr_sem.at[half],
            {"tensor": other},
        )

    targets = [
        lookup(place, [send_order(p, owners)[k] for p in range(owners)]) for k in range(owners)
    ]
    sources = [
        lookup(place, [arrival_order(p, owners)[k] for p in range(owners)]) for k in range(owners)
    ]

    for k in range(1, owners):
        for tile in range(tiles):
            push(
                proj_ref.at[targets[k], tile],
                out_ref.at[mine, place, tile],
                zs_sem.at[k, tile],
                zr_sem.at[place, tile],
                {"seq": targets[k]},
            )

    def spread(src, k, tile):
        owner = sources[k]
        for step in range(1, chips):
            other = (chip + step) % chips
            push(
                src,
                out_ref.at[mine, owner, tile],
                xs_sem.at[step, k, tile],
                xr_sem.at[chip, owner, tile],
                {"dp": other * CORES + core},
            )
        push(
            src,
            out_ref.at[mine, owner, tile],
            cs_sem.at[0, k, tile],
            cr_sem.at[chip, owner, tile],
            {"dp": partner},
        )

    def relay(k, tile):
        owner = sources[k]
        for step in range(1, chips):
            other = (chip + chips - step) % chips
            origin = other * CORES + core
            block = out_ref.at[origin, owner, tile]
            arrived(block, xs_sem.at[step, k, tile], xr_sem.at[other, owner, tile], {"dp": origin})
            push(
                block,
                block,
                cs_sem.at[step, k, tile],
                cr_sem.at[other, owner, tile],
                {"dp": partner},
            )

    for tile in range(tiles):
        spread(proj_ref.at[place, tile], 0, tile)
    keep = pltpu.make_async_copy(proj_ref.at[place], out_ref.at[mine, place], local_sem)
    keep.start()

    total = stat_ref[...]
    for step in range(1, splits):
        other = (half + step) % splits
        arrived(y_land.at[other], ys_sem.at[step], yr_sem.at[other], {"tensor": other})
        total = total + y_land[other]
    z_land[place] = total
    for step in range(1, owners):
        other = (place + step) % owners
        push(
            z_land.at[place],
            z_land.at[place],
            zss_sem.at[step],
            zsr_sem.at[place],
            {"seq": other},
        )

    def statistics():
        text_total = jnp.zeros(text_ref.shape, jnp.float32)
        for step in range(1, owners):
            other = (place + step) % owners
            arrived(z_land.at[other], zss_sem.at[step], zsr_sem.at[other], {"seq": other})
        for owner in range(owners):
            text_total = text_total + z_land[owner, STAT_ROWS:, :]
            d_land[mine, owner] = z_land[owner, :STAT_ROWS, :]
        text_ref[...] = text_total
        for step in range(1, replicas):
            other = (mine + step) % replicas
            push(
                d_land.at[mine],
                d_land.at[mine],
                ds_sem.at[step],
                dr_sem.at[mine],
                {"dp": other},
            )

    for k in range(1, owners):
        for tile in range(tiles):
            arrived(
                out_ref.at[mine, sources[k], tile],
                zs_sem.at[k, tile],
                zr_sem.at[sources[k], tile],
                {"seq": sources[k]},
            )
            spread(out_ref.at[mine, sources[k], tile], k, tile)
        if k == owners - 1:
            statistics()
        for tile in range(tiles):
            relay(k - 1, tile)
    for tile in range(tiles):
        relay(owners - 1, tile)

    for step in range(1, replicas):
        other = (mine + step) % replicas
        arrived(d_land.at[other], ds_sem.at[step], dr_sem.at[other], {"dp": other})
    vision_ref[...] = d_land[...]
    for k in range(owners):
        for other in range(chips):
            origin = other * CORES + 1 - core
            for tile in range(tiles):
                arrived(
                    out_ref.at[origin, sources[k], tile],
                    cs_sem.at[0, k, tile],
                    cr_sem.at[other, sources[k], tile],
                    {"dp": partner},
                )
    keep.wait()
    for copy in sends:
        copy.wait_send()


def exchange(blocks, stats, sizes):
    replicas, owners, splits, tiles = sizes
    chips = replicas // CORES
    columns = blocks.shape[-1]
    rows = stats.shape[0]
    dma = pltpu.SemaphoreType.DMA
    return pl.pallas_call(
        functools.partial(exchange_kernel, sizes),
        out_shape=(
            jax.ShapeDtypeStruct((replicas, owners, tiles, TILE, columns), jnp.bfloat16),
            jax.ShapeDtypeStruct((rows - STAT_ROWS, TILE), jnp.float32),
            jax.ShapeDtypeStruct((replicas, owners, STAT_ROWS, TILE), jnp.float32),
        ),
        in_specs=[pl.BlockSpec(memory_space=pltpu.VMEM)] * 2,
        out_specs=(
            pl.BlockSpec(memory_space=pl.ANY),
            pl.BlockSpec(memory_space=pltpu.VMEM),
            pl.BlockSpec(memory_space=pltpu.VMEM),
        ),
        scratch_shapes=[
            pltpu.VMEM((splits, rows, TILE), jnp.float32),
            pltpu.VMEM((owners, rows, TILE), jnp.float32),
            pltpu.VMEM((replicas, owners, STAT_ROWS, TILE), jnp.float32),
            dma,
            dma((owners, tiles)),
            dma((owners, tiles)),
            dma((chips, owners, tiles)),
            dma((chips, owners, tiles)),
            dma((chips, owners, tiles)),
            dma((chips, owners, tiles)),
            dma((splits,)),
            dma((splits,)),
            dma((owners,)),
            dma((owners,)),
            dma((replicas,)),
            dma((replicas,)),
        ],
        compiler_params=pltpu.CompilerParams(collective_id=0, has_side_effects=True),
        name="exchange",
    )(blocks, stats)


def tile_squares(values, rows):
    columns = values.shape[1]
    part = jnp.zeros((rows, TILE), jnp.float32)
    for start in range(0, columns, TILE):
        lanes = values[:, start : start + TILE].astype(jnp.float32)
        part = part + lanes * lanes
    return part


def project_kernel(
    depth,
    text_steps,
    rows_ref,
    weight_ref,
    bias_ref,
    text_ref,
    block_ref,
    own_ref,
    text_out,
    total,
):
    step = pl.program_id(0)
    owners, tiles, _, columns = block_ref.shape

    @pl.when(step == 0)
    def _():
        own_ref[...] = jnp.zeros_like(own_ref)

    for owner in range(owners):
        term = jnp.dot(
            rows_ref[...], weight_ref[:, owner * columns : (owner + 1) * columns], preferred_element_type=jnp.float32
        )

        @pl.when(step == 0)
        def _():
            total[owner] = term + bias_ref[pl.ds(owner, 1), :]

        @pl.when(step > 0)
        def _():
            total[owner] += term

    @pl.when(step < text_steps)
    def _():
        for item in range(text_out.shape[0]):
            part = tile_squares(text_ref[item * TILE : (item + 1) * TILE, :], TILE)
            text_out[item] = jnp.sum(part.T, axis=0, keepdims=True)

    @pl.when(step == depth - 1)
    def _():
        for tile in range(tiles):
            part = jnp.zeros((TILE, TILE), jnp.float32)
            for owner in range(owners):
                values = total[owner, tile * TILE : (tile + 1) * TILE, :].astype(jnp.bfloat16)
                block_ref[owner, tile] = values
                part = part + tile_squares(values, TILE)
            own_ref[tile : tile + 1, :] = jnp.sum(part.T, axis=0, keepdims=True)


def project(rows, weight, bias, text_embed, positions):
    count, width = rows.shape
    owners, columns = weight.shape[1:]
    flat = weight.reshape(width, owners * columns)
    tiles = count // TILE
    cut = max(c for c in range(TILE, DEPTH + 1, TILE) if width % c == 0)
    depth = width // cut
    text_steps = max(c for c in range(1, depth + 1) if positions % c == 0)
    group = positions // text_steps
    last = text_steps - 1
    return pl.pallas_call(
        functools.partial(project_kernel, depth, text_steps),
        grid=(depth,),
        in_specs=[
            pl.BlockSpec((count, cut), lambda step: (0, step)),
            pl.BlockSpec((cut, owners * columns), lambda step: (step, 0)),
            pl.BlockSpec(bias.shape, lambda step: (0, 0)),
            pl.BlockSpec((group * TILE, columns), lambda step: (jnp.minimum(step, last), 0)),
        ],
        out_specs=(
            pl.BlockSpec((owners, tiles, TILE, columns), lambda step: (0, 0, 0, 0)),
            pl.BlockSpec((STAT_ROWS, TILE), lambda step: (0, 0)),
            pl.BlockSpec((group, 1, TILE), lambda step: (jnp.minimum(step, last), 0, 0)),
        ),
        out_shape=(
            jax.ShapeDtypeStruct((owners, tiles, TILE, columns), jnp.bfloat16),
            jax.ShapeDtypeStruct((STAT_ROWS, TILE), jnp.float32),
            jax.ShapeDtypeStruct((positions, 1, TILE), jnp.float32),
        ),
        scratch_shapes=[pltpu.VMEM((owners, count, columns), jnp.float32)],
        compiler_params=pltpu.CompilerParams(vmem_limit_bytes=50 * 2**20),
        name="project",
    )(rows, flat, bias, text_embed)


def place_kernel(group, width, source_ref, *refs):
    picked = refs[:group]
    text_ref, text_sum, vision_sum, gain_ref, out_ref = refs[group:]
    first = pl.program_id(0) * group
    gain = gain_ref[...]
    for item in range(group):
        source = source_ref[first + item]
        rows = slice(item * TILE, (item + 1) * TILE)

        def scaled(values, squares):
            scale = lax.rsqrt(squares / width + 1e-05)
            column = jnp.broadcast_to(scale, (TILE, TILE)).T
            for start in range(0, out_ref.shape[1], TILE):
                lanes = slice(start, start + TILE)
                out_ref[rows, lanes] = (
                    values[:, lanes].astype(jnp.float32) * column * gain[:, lanes]
                ).astype(jnp.bfloat16)

        @pl.when(source >= 0)
        def _():
            scaled(picked[item][0], vision_sum[pl.ds(source, 1), :])

        @pl.when(source < 0)
        def _():
            scaled(text_ref[rows, :], text_sum[pl.ds(first + item, 1), :])


def place(source_tile, gathered, text_embed, text_sum, vision_sum, norm_gain, width):
    positions = source_tile.shape[0]
    group = 4
    columns = text_embed.shape[1]

    def pick(item):
        return lambda step, source: (jnp.maximum(source[step * group + item], 0), 0, 0)

    whole = lambda step, source: (0, 0)
    return pl.pallas_call(
        functools.partial(place_kernel, group, width),
        grid_spec=pltpu.PrefetchScalarGridSpec(
            num_scalar_prefetch=1,
            grid=(positions // group,),
            in_specs=[pl.BlockSpec((1, TILE, columns), pick(item)) for item in range(group)]
            + [
                pl.BlockSpec((group * TILE, columns), lambda step, source: (step, 0)),
                pl.BlockSpec(text_sum.shape, whole),
                pl.BlockSpec(vision_sum.shape, whole),
                pl.BlockSpec((1, columns), whole),
            ],
            out_specs=pl.BlockSpec((group * TILE, columns), lambda step, source: (step, 0)),
        ),
        out_shape=jax.ShapeDtypeStruct(text_embed.shape, jnp.bfloat16),
        name="place",
    )(source_tile, *([gathered] * group), text_embed, text_sum, vision_sum, norm_gain[None, :])


def local(
    vit_out, ln_gain, ln_bias, proj_weight, proj_bias, text_embed, norm_gain, tile_dest, tile_place
):
    replicas = lax.axis_size("dp")
    owners = lax.axis_size("seq")
    splits = lax.axis_size("tensor")
    mine = lax.axis_index("dp")
    local_rows = vit_out.shape[0]
    columns = proj_weight.shape[2]
    positions = tile_place.shape[1]
    total_tiles = tile_dest.shape[0]
    tiles = local_rows // TILE
    sizes = (replicas, owners, splits, tiles)

    normed_in = layer_norm(vit_out, ln_gain, ln_bias)
    blocks, own_squares, text_squares = project(
        normed_in, proj_weight, proj_bias, text_embed, positions
    )
    stats = jnp.concatenate([own_squares, text_squares.reshape(positions, TILE)])
    gathered, text_sum, vision_sum = exchange(blocks, stats, sizes)

    named = tile_dest[:, 0] == mine
    earlier = jnp.arange(total_tiles)[None, :] < jnp.arange(total_tiles)[:, None]
    ranks = jnp.sum((earlier & named[None, :]).astype(jnp.int32), axis=1)
    place_row = lax.dynamic_index_in_dim(tile_place, mine, 0, keepdims=False)
    numbers = jnp.arange(positions, dtype=jnp.int32)
    order = jnp.sum(
        jnp.where(place_row[None, :] == numbers[:, None], numbers[None, :], 0), axis=1
    )
    matches = named[None, :] & (ranks[None, :] == order[:, None])
    source_tile = jnp.max(
        jnp.where(matches, jnp.arange(total_tiles, dtype=jnp.int32)[None, :], -1), axis=1
    )
    return place(
        source_tile,
        gathered.reshape(total_tiles, TILE, columns),
        text_embed,
        text_sum,
        vision_sum[:, :, :tiles, :].reshape(total_tiles, TILE),
        norm_gain,
        norm_gain.shape[0] * owners * splits,
    )


def solution(mesh):
    placed = (
        P(("dp", "seq"), None),
        P(),
        P(),
        P(None, None, "tensor"),
        P(None, "tensor"),
        P("dp", ("seq", "tensor")),
        P(("seq", "tensor")),
        P(),
        P(),
    )
    return jax.shard_map(
        local, mesh=mesh, in_specs=placed, out_specs=P("dp", ("seq", "tensor")), check_vma=False
    )
```
